32 devices in a mesh: shot: 8 (over z, x), freq: 4 (over y, core).
Axes of the slice: x: 2, y: 2, z: 4, core: 2. Of those that a mesh axis runs over, the one named last changes fastest.
Arguments:
- traces: float32 [4, 2, 32768], P('freq', None, 'shot'), may hold values from -6 to 6
- trace_slot: int32 [32768], P('shot'), may hold values from 0 to 8191, as said below
- trace_cmp: int32 [32768], P('shot'), may hold values from 0 to 3
- trace_bin: int32 [32768], P('shot'), may hold values from 0 to 511
- prior_weight: float32 [128, 256], P('shot'), may hold values from 0.5 to 2
Outputs:
- primaries: float32 [4, 2, 32768], P('freq', None, 'shot')
- radon_model: float32 [4, 2, 128, 256], P('freq', None, 'shot')
The draws below stay inside these ranges and needn't reach their ends.
Inputs may be any that keep to these rules, and one draw needn't show every extreme that they name: On each index of shot the values are distinct; trace_slot // 256 is the owning shot index of the trace's CMP gather times 4 plus the quarter of that owner's gathers, so at most 256 traces of one index of shot go to one quarter of one owner; in every draw one such quarter receives exactly 256 traces from every index of shot.
All inputs are finite; a program needn't handle non-finite values.
Results may differ from the reference program's by a relative error of at most 0.0085.
Values sent between devices are 32-bit elements; how exact they have to be, the bound alone decides.
No kernel may reach another device: no remote copies, remote signals or barrier semaphores. Data moves between devices by JAX's collectives and lax.ppermute only.
A program may use at most 64 MiB of HBM per device.

```python
import math
import jax
import jax.numpy as jnp
from jax import lax

BINS = 512
Q = 256
CG_STEPS = 8
IRLS = 2
TR_DEV = 4096
FREQS = 4
CMPS = 128
CMP_Q = 4
CAPQ = 256
TRACES = 32768
N_SHOT = 8
N_FREQ = 4


def draw_trace_slot(key, part):
    slot_total = N_SHOT * N_FREQ * CAPQ
    group_total = N_SHOT * N_FREQ
    full_group = jax.random.randint(jax.random.fold_in(key, 11), (), 0, group_total)
    favour = jax.random.randint(jax.random.fold_in(key, 12), (group_total,), 0, 4)
    slot_group = jnp.arange(slot_total, dtype=jnp.int32) // CAPQ
    base_score = -favour[slot_group] * 65536
    base_score = jnp.where(slot_group == full_group, -(1 << 22), base_score)

    def one_device(device):
        device_key = jax.random.fold_in(jax.random.fold_in(key, 13), device)
        jitter = jax.random.randint(device_key, (slot_total,), 0, 1 << 18)
        ranking = jnp.argsort(base_score + jitter, stable=True)
        chosen = ranking[:TR_DEV].astype(jnp.int32)
        return jax.random.permutation(jax.random.fold_in(device_key, 5), chosen)
    return jax.vmap(one_device)(jnp.arange(N_SHOT, dtype=jnp.int32)).reshape(-1).astype(jnp.int32)


def touch_ends(values, stream_key, smallest, top_value):
    shape = values.shape
    place = [jax.random.randint(jax.random.fold_in(stream_key, axis), (), 0, shape[axis]) for axis in range(len(shape))]
    values = values.at[tuple(place)].set(smallest)
    longest = shape.index(max(shape))
    place[longest] = (place[longest] + 1) % shape[longest]
    return values.at[tuple(place)].set(top_value)


def steps_of(key, extent, split, least, largest):
    def one(dim, shards_of):
        heights = jax.random.uniform(jax.random.fold_in(jax.random.fold_in(key, 6), dim), (shards_of,), jnp.float32, least / len(split), largest / len(split))
        return jnp.repeat(jnp.exp(heights), extent[dim] // shards_of).reshape((-1,) + (1,) * (len(extent) - dim - 1))

    factor_of = one(*split[0])
    for cut in split[1:]:
        factor_of = factor_of * one(*cut)
    return factor_of


def noise(own_key, dims, scale, bound, shards=(), kind=jnp.bfloat16):
    result = scale * jax.random.normal(own_key, dims, jnp.float32)
    if shards:
        result = result * steps_of(own_key, dims, shards, -0.22, 0.18)
    return jnp.clip(result, -bound, bound).astype(kind)


def setup_inputs(seed: int = 0) -> dict:
    streams_of = jax.random.split(jax.random.key(seed), 6)
    return {
        "traces": noise(streams_of[0], (FREQS, 2, TRACES), 1.0, 6.0, ((0, 4), (2, 8)), jnp.float32),
        "trace_slot": draw_trace_slot(jax.random.fold_in(streams_of[5], 71), 0),
        "trace_cmp": touch_ends(jax.random.randint(streams_of[2], (TRACES,), 0, CMP_Q), jax.random.fold_in(streams_of[2], 1), 0, CMP_Q - 1).astype(jnp.int32),
        "trace_bin": touch_ends(jax.random.randint(streams_of[3], (TRACES,), 0, BINS), jax.random.fold_in(streams_of[3], 1), 0, BINS - 1).astype(jnp.int32),
        "prior_weight": jnp.clip(jnp.exp(math.log(2.0) - 1.3862944 * jax.random.uniform(streams_of[4], (CMPS, Q), jnp.float32) ** steps_of(streams_of[4], (CMPS, Q), ((0, 8),), -0.2, 0.2)), 0.5, 2.0),
    }


MU_SCALE = 0.5
ENERGY_FLOOR = 0.5
SMALL_EPS = 1e-6


def radon_table(freq_ids, freq_total):
    nu_value = 0.5 + 0.5 * freq_ids.astype(jnp.float32) / freq_total
    curvature = jnp.arange(Q).astype(jnp.float32) - (Q // 8)
    offset = (jnp.arange(BINS).astype(jnp.float32) + 0.5) / BINS
    phase = (2.0 * math.pi) * nu_value[:, None, None] * curvature[None, :, None] * (offset * offset)[None, None, :]
    return jnp.cos(phase), -jnp.sin(phase)


def spread(operand, table_part):
    return jnp.einsum('fcq,fqb->fcb', operand, table_part, precision=lax.Precision.HIGHEST)


def collect(operand, table_part):
    return jnp.einsum('fcb,fqb->fcq', operand, table_part, precision=lax.Precision.HIGHEST)


def forward(field, cos_table, sin_table):
    real_part = spread(field[:, 0], cos_table) - spread(field[:, 1], sin_table)
    imag_part = spread(field[:, 1], cos_table) + spread(field[:, 0], sin_table)
    return jnp.stack([real_part, imag_part], axis=1)


def adjoint(binned, cos_table, sin_table):
    real_part = collect(binned[:, 0], cos_table) + collect(binned[:, 1], sin_table)
    imag_part = collect(binned[:, 1], cos_table) - collect(binned[:, 0], sin_table)
    return jnp.stack([real_part, imag_part], axis=1)


def inner_sum(first, second):
    return jnp.sum(first * second, axis=(1, 3))[:, None, :, None]


def conjugate(right_side, counts, weight, cos_table, sin_table):
    damping = MU_SCALE * BINS * weight[None, None]
    fold_map = counts[None, None]
    solution = jnp.zeros_like(right_side)
    residual = right_side
    direction = right_side
    norm_now = inner_sum(residual, residual)
    for cg_step in range(CG_STEPS):
        image_vec = adjoint(fold_map * forward(direction, cos_table, sin_table), cos_table, sin_table) + damping * direction
        step_size = norm_now / inner_sum(direction, image_vec)
        solution = solution + step_size * direction
        residual = residual - step_size * image_vec
        norm_next = inner_sum(residual, residual)
        direction = residual + (norm_next / norm_now) * direction
        norm_now = norm_next
    return solution


def reweigh(energy):
    average = jnp.mean(energy, axis=1, keepdims=True)
    return (average + SMALL_EPS) / (energy + ENERGY_FLOOR * average + SMALL_EPS)


def reference(traces, trace_slot, trace_cmp, trace_bin, prior_weight):
    cell_index = ((trace_slot // CAPQ) * CMP_Q + trace_cmp) * BINS + trace_bin
    flat = traces.reshape(FREQS * 2, TRACES).T
    binned = jax.ops.segment_sum(flat, cell_index, num_segments=CMPS * BINS).T.reshape(FREQS, 2, CMPS, BINS)
    counts = jax.ops.segment_sum(jnp.ones((TRACES,), jnp.float32), cell_index, num_segments=CMPS * BINS).reshape(CMPS, BINS)
    cos_table, sin_table = radon_table(jnp.arange(FREQS, dtype=jnp.int32), FREQS)
    right_side = adjoint(binned, cos_table, sin_table)
    weight = prior_weight
    radon_model = right_side
    for irls_pass in range(IRLS):
        if irls_pass > 0:
            weight = reweigh(jnp.sum(radon_model * radon_model, axis=(0, 1)))
        radon_model = conjugate(right_side, counts, weight, cos_table, sin_table)
    multiple_mask = (jnp.arange(Q) >= Q // 4).astype(jnp.float32)
    predicted = forward(radon_model * multiple_mask, cos_table, sin_table).reshape(FREQS, 2, CMPS * BINS)
    primaries = traces - predicted[:, :, cell_index]
    return primaries, radon_model
```

```python
import math
from functools import partial

import numpy as np
import jax
import jax.numpy as jnp
from jax import lax
from jax.experimental import pallas as pl
from jax.experimental.pallas import tpu as pltpu
from jax.sharding import PartitionSpec as P

BINS = 512
Q = 256
CG_STEPS = 8
IRLS = 2

MU_SCALE = 0.5
ENERGY_FLOOR = 0.5
SMALL_EPS = 1e-06

LANES = 128
BLOCK = 256
HALF = Q // 2
RADIX = 4
INTERPRET = False

F32 = jnp.float32
BF16 = jnp.bfloat16
NT = (((1,), (1,)), ((), ()))
NN = (((1,), (0,)), ((), ()))


def halves_of(value):
    high = value.astype(BF16)
    return high, (value - high.astype(F32)).astype(BF16)


def thirds_of(value):
    high = value.astype(BF16)
    return high, *halves_of(value - high.astype(F32))


def matmul(left, right, dims):
    return lax.dot_general(left, right, dims, preferred_element_type=F32)


def sublane(shape):
    return lax.broadcasted_iota(jnp.int32, shape, 0)


def np_thirds(value):
    parts = []
    for _ in range(3):
        part = value.astype(np.float32).astype(jnp.bfloat16)
        parts.append(part)
        value = value - part.astype(np.float64)
    return parts


def dft_constants():
    index = np.arange(HALF)
    angle = -2.0 * np.pi * ((index[:, None] * index[None, :]) % HALF) / HALF
    real, imag = np.cos(angle), np.sin(angle)
    ahead = np.block([[real, imag], [-imag, real]])
    dft = np.concatenate([*np_thirds(ahead), *np_thirds(ahead.T)], axis=0)
    twiddle = np.zeros((8, HALF))
    for r in range(1, RADIX):
        twiddle[2 * r] = np.cos(2.0 * np.pi * index * r / (RADIX * HALF))
        twiddle[2 * r + 1] = -np.sin(2.0 * np.pi * index * r / (RADIX * HALF))
    return jnp.asarray(dft), jnp.asarray(twiddle.astype(np.float32))


def phase_constants(freq_total):
    steps = np.concatenate([np.arange(16), 16 * np.arange(Q // 16)])
    squares = (2 * np.arange(BINS, dtype=np.int64) + 1) ** 2
    whole = 2 * freq_total * 4 * BINS * BINS
    rows = []
    for f in range(freq_total):
        turns = ((freq_total + f) * steps[:, None] * squares[None, :]) % whole
        angle = 2.0 * np.pi * turns / whole
        rows.append(np.concatenate([np.cos(angle), np.sin(angle)], axis=0))
    return jnp.asarray(np.stack(rows).astype(np.float32))


def held(*arrays):
    return [pltpu.with_memory_space_constraint(a, pltpu.HBM) for a in arrays]


def fetch(sources, targets, sems):
    copies = [pltpu.make_async_copy(a, b, sems.at[n]) for n, (a, b) in enumerate(zip(sources, targets))]
    for copy in copies:
        copy.start()
    return copies


def route_kernel(traces_hbm, slot_hbm, cmp_hbm, bin_hbm, out_ref, traces_ref, slot_ref, cmp_ref, bin_ref, sems):
    sources = (slot_hbm, traces_hbm, cmp_hbm, bin_hbm)
    for copy in fetch(sources, (slot_ref, traces_ref, cmp_ref, bin_ref), sems):
        copy.wait()
    blocks = out_ref.shape[0]
    total = slot_ref.shape[1]
    width = min(1024, total)
    acc = jnp.zeros((3 * 8 * blocks, LANES), F32)
    for start in range(0, total, width):
        part = slice(start, start + width)
        slot = slot_ref[:, part]
        label = (1 + cmp_ref[:, part] * BINS + bin_ref[:, part]).astype(F32)
        shape = (8, width)
        row = sublane(shape)
        value = jnp.where(row < 2, traces_ref[0:1, part], traces_ref[1:2, part])
        value = jnp.where(row < 4, value, jnp.where(row < 6, label, 0.0))
        key = jnp.where((slot // LANES) % 2 == row % 2, slot // BLOCK, -1)
        onehot = jnp.where(sublane((LANES, width)) == slot % LANES, 1.0, 0.0).astype(BF16)
        lefts = []
        for third in thirds_of(value):
            third = third.astype(F32)
            for d in range(blocks):
                lefts.append(jnp.where(key == d, third, 0.0))
        left = jnp.concatenate(lefts, axis=0).astype(BF16)
        acc = acc + matmul(left, onehot, NT)
    rows = 8 * blocks
    acc = acc[:rows] + (acc[rows : 2 * rows] + acc[2 * rows :])
    out_ref[...] = acc.reshape(blocks, 8, LANES)


def unroute_kernel(traces_ref, slot_ref, back_ref, *refs):
    *model_refs, out_ref, radon_ref, stage_ref = refs
    total = slot_ref.shape[1]
    rows = back_ref.shape[0]
    width = min(1024, total)
    left = jnp.concatenate(halves_of(back_ref[...]), axis=0)
    for start in range(0, total, width):
        part = slice(start, start + width)
        slot = slot_ref[:, part]
        onehot = jnp.where(sublane((LANES, width)) == slot % LANES, 1.0, 0.0).astype(BF16)
        wide = matmul(left, onehot, NN)
        wide = wide[:rows] + wide[rows:]
        row = sublane((8, width))
        key = slot // LANES - ((row // 4) * 2 + row % 2)
        acc = jnp.zeros((8, width), F32)
        for g in range(rows // 8):
            acc = acc + jnp.where(key == 4 * g, wide[8 * g : 8 * g + 8], 0.0)
        acc = acc + pltpu.roll(acc, 1, 0)
        acc = acc + pltpu.roll(acc, 4, 0)
        out_ref[0:1, part] = traces_ref[0:1, part] - acc[1:2]
        out_ref[1:2, part] = traces_ref[1:2, part] - acc[3:4]
    owner = lax.axis_index("freq")
    for k, model_ref in enumerate(model_refs):
        stage_ref[jnp.bitwise_xor(owner, k)] = model_ref[...]
    quarter = stage_ref.shape[1] // 2
    for j in range(len(model_refs)):
        for p in range(2):
            radon_ref[p, j * quarter : (j + 1) * quarter, :] = stage_ref[j, p * quarter : (p + 1) * quarter, :]


def split_dot(left, high, low, dims):
    rows = left.shape[0]
    first, second = halves_of(left)
    both = matmul(jnp.concatenate([first, second], axis=0), high, dims)
    return both[:rows] + both[rows:] + matmul(first, low, dims)


def sharp_dot(left, high, low, dims):
    rows = left.shape[0]
    first, second, third = thirds_of(left)
    one = matmul(jnp.concatenate([first, second, third], axis=0), high, dims)
    two = matmul(jnp.concatenate([first, second], axis=0), low, dims)
    return one[:rows] + (one[rows : 2 * rows] + two[:rows] + (one[2 * rows :] + two[rows:]))


def fine_dot(left, table_ref, place):
    rows = left.shape[0]
    first, second, third = thirds_of(left)
    high, middle, low = (table_ref[place + k * Q : place + (k + 1) * Q] for k in range(3))
    one = matmul(jnp.concatenate([first, second, third], axis=0), high, NN)
    two = matmul(jnp.concatenate([first, second], axis=0), middle, NN)
    small = two[rows:] + (one[2 * rows :] + matmul(first, low, NN))
    return one[:rows] + (one[rows : 2 * rows] + two[:rows] + small)


def spectrum(real, imag, dft_ref, tw_ref):
    ar, br = real[:, :HALF], real[:, HALF:]
    ai, bi = imag[:, :HALF], imag[:, HALF:]
    sums = [(ar + br, ai + bi), (ar + bi, ai - br), (ar - br, ai - bi), (ar - bi, ai + br)]
    reals, imags = [sums[0][0]], [sums[0][1]]
    for r in range(1, RADIX):
        c, s = tw_ref[2 * r : 2 * r + 1, :], tw_ref[2 * r + 1 : 2 * r + 2, :]
        u, v = sums[r]
        reals.append(c * u - s * v)
        imags.append(c * v + s * u)
    left = jnp.concatenate([jnp.concatenate(reals, axis=0), jnp.concatenate(imags, axis=0)], axis=1)
    return fine_dot(left, dft_ref, 0)


def unspectrum(values, dft_ref, tw_ref):
    rows = values.shape[0] // RADIX
    both = fine_dot(values, dft_ref, 3 * Q)
    zs = []
    for r in range(RADIX):
        u, v = both[r * rows : (r + 1) * rows, :HALF], both[r * rows : (r + 1) * rows, HALF:]
        if r:
            c, s = tw_ref[2 * r : 2 * r + 1, :], tw_ref[2 * r + 1 : 2 * r + 2, :]
            u, v = c * u + s * v, c * v - s * u
        zs.append((u, v))
    real = [zs[0][0] + zs[2][0] + (zs[1][0] + zs[3][0]), zs[0][0] - zs[2][0] - (zs[1][1] - zs[3][1])]
    imag = [zs[0][1] + zs[2][1] + (zs[1][1] + zs[3][1]), zs[0][1] - zs[2][1] + (zs[1][0] - zs[3][0])]
    return jnp.concatenate(real, axis=1), jnp.concatenate(imag, axis=1)


def dot_rows(ar, ai, br, bi):
    return jnp.sum(ar * br + ai * bi, axis=1, keepdims=True)


def conjugate(rhs, first, damping, fold, dft_ref, tw_ref):
    def image_of(dr, di, wave):
        yr, yi = unspectrum(wave * fold, dft_ref, tw_ref)
        return yr + damping * dr, yi + damping * di

    def step(_, state):
        sr, si, rr, ri, dr, di, residual_wave, wave, norm = state
        mr, mi = image_of(dr, di, wave)
        image_wave = spectrum(mr, mi, dft_ref, tw_ref)
        alpha = norm / dot_rows(dr, di, mr, mi)
        sr, si = sr + alpha * dr, si + alpha * di
        rr, ri = rr - alpha * mr, ri - alpha * mi
        new = dot_rows(rr, ri, rr, ri)
        beta = new / norm
        alphas = jnp.concatenate([alpha] * RADIX, axis=0)
        betas = jnp.concatenate([beta] * RADIX, axis=0)
        residual_wave = residual_wave - alphas * image_wave
        return sr, si, rr, ri, rr + beta * dr, ri + beta * di, residual_wave, residual_wave + betas * wave, new

    br, bi = rhs
    zero = jnp.zeros_like(br)
    state = (zero, zero, br, bi, br, bi, first, first, dot_rows(br, bi, br, bi))
    sr, si, rr, ri, dr, di, _, wave, norm = lax.fori_loop(0, CG_STEPS - 1, step, state)
    mr, mi = image_of(dr, di, wave)
    alpha = norm / dot_rows(dr, di, mr, mi)
    return sr + alpha * dr, si + alpha * di


def swap(value):
    return pltpu.roll(value, 4, 0)


def solve_kernel(in_ref, prior_ref, tw_ref, base_hbm, dft_hbm, out_ref, *refs):
    *model_refs, left_ref, hot_ref, high_ref, low_ref, base_ref, dft_ref, stage_ref, sems = refs
    base_copy, dft_copy = fetch((base_hbm, dft_hbm), (base_ref, dft_ref), sems)
    freqs = base_ref.shape[0]
    shots = in_ref.shape[0] // freqs
    parts = BINS // LANES
    row = sublane((8, LANES))
    lane_row = sublane((LANES, LANES))

    def cells(s, h):
        cell = in_ref[s * freqs, 4 + h : 5 + h, :].astype(jnp.int32) - 1
        return (cell >> 7) - 4 * (row % 4), cell & (LANES - 1)

    for s in range(shots):
        for h in range(2):
            lanes = slice((2 * s + h) * LANES, (2 * s + h + 1) * LANES)
            key, low_index = cells(s, h)
            hot_ref[:, lanes] = jnp.where(lane_row == low_index, 1.0, 0.0).astype(BF16)
            thirds = [], [], []
            for f in range(freqs):
                value = jnp.where(row < 4, in_ref[s * freqs + f, h : h + 1, :], in_ref[s * freqs + f, 2 + h : 3 + h, :])
                for group, third in zip(thirds, thirds_of(value)):
                    group.append(third.astype(F32))
            rows = []
            for group in (*thirds, [jnp.ones((8, LANES), F32)]):
                for part in range(parts):
                    for value in group:
                        rows.append(jnp.where(key == part, value, 0.0))
            left_ref[:, lanes] = jnp.concatenate(rows, axis=0).astype(BF16)
    sums = matmul(left_ref[...], hot_ref[...], NT)
    half = parts * freqs * 8
    binned = sums[:half] + (sums[half : 2 * half] + sums[2 * half : 3 * half])
    counts = jnp.concatenate([sums[3 * half + 8 * k : 3 * half + 8 * k + 8] for k in range(parts)], axis=1)

    base_copy.wait()
    sign = jnp.where(sublane((8, 1)) < 4, 1.0, -1.0)
    right_real, right_imag, fold_real, fold_imag = [], [], [], []
    for f in range(freqs):
        near_cos, near_sin = base_ref[f, 0:16, :], base_ref[f, 32:48, :]
        for k in range(Q // 16):
            far_cos, far_sin = base_ref[f, 16 + k : 17 + k, :], base_ref[f, 48 + k : 49 + k, :]
            for place, value in (
                (16 * k, near_cos * far_cos - near_sin * far_sin),
                (Q + 16 * k, near_sin * far_cos + near_cos * far_sin),
            ):
                high, low = halves_of(value)
                high_ref[f, place : place + 16, :] = high
                low_ref[f, place : place + 16, :] = low
        shift = 16 + (Q // 8) // 16
        shift_cos, shift_sin = base_ref[f, shift : shift + 1, :], base_ref[f, 32 + shift : 33 + shift, :]
        field = jnp.concatenate([binned[(k * freqs + f) * 8 : (k * freqs + f) * 8 + 8] for k in range(parts)], axis=1)
        field = field * shift_cos + swap(field) * (sign * shift_sin)
        both = sharp_dot(jnp.concatenate([field, counts], axis=0), high_ref[f], low_ref[f], NT)
        right = both[:8, :Q] - sign * swap(both[:8, Q:])
        right_real.append(right[:4])
        right_imag.append(right[4:])
        fold_real.append(both[8:12, :Q])
        fold_imag.append(both[8:12, Q:])
    rhs = jnp.concatenate(right_real, axis=0), jnp.concatenate(right_imag, axis=0)
    fold_real, fold_imag = jnp.concatenate(fold_real, axis=0), jnp.concatenate(fold_imag, axis=0)
    lane = lax.broadcasted_iota(jnp.int32, fold_real.shape, 1)
    fold_real = jnp.where(lane == 0, 0.5, 1.0) * fold_real
    fold_imag = jnp.where(lane == 0, 0.0, fold_imag)
    dft_copy.wait()
    fold = spectrum(fold_real, fold_imag, dft_ref, tw_ref)[:, :HALF] * (2.0 / (RADIX * HALF))
    fold = jnp.concatenate([fold, fold], axis=1)

    first = spectrum(*rhs, dft_ref, tw_ref)
    owner = lax.axis_index("freq")
    weight = prior_ref[0:4, :]
    for j in range(1, freqs):
        weight = jnp.where(owner == j, prior_ref[4 * j : 4 * j + 4, :], weight)
    weight = jnp.concatenate([weight] * freqs, axis=0)
    for irls_pass in range(IRLS):
        if irls_pass:
            power = model[0] * model[0] + model[1] * model[1]
            energy = power[0:8]
            for k in range(1, freqs // 2):
                energy = energy + power[8 * k : 8 * k + 8]
            energy = energy + swap(energy)
            average = jnp.mean(energy, axis=1, keepdims=True)
            weight = (average + SMALL_EPS) / (energy + ENERGY_FLOOR * average + SMALL_EPS)
            weight = jnp.concatenate([weight] * (freqs // 2), axis=0)
        model = conjugate(rhs, first, (MU_SCALE * BINS) * weight, fold, dft_ref, tw_ref)

    wides = []
    multiple = lax.broadcasted_iota(jnp.int32, (8, Q), 1) >= Q // 4
    for f in range(freqs):
        field = jnp.concatenate([model[0][4 * f : 4 * f + 4], model[1][4 * f : 4 * f + 4]], axis=0)
        stage_ref[f] = field
        field = jnp.where(multiple, field, 0.0)
        cos_part = split_dot(field, high_ref[f, :Q, :], low_ref[f, :Q, :], NN)
        sin_part = split_dot(field, high_ref[f, Q:, :], low_ref[f, Q:, :], NN)
        value = cos_part + sign * swap(sin_part)
        shift = 16 + (Q // 8) // 16
        shift_cos, shift_sin = base_ref[f, shift : shift + 1, :], base_ref[f, 32 + shift : 33 + shift, :]
        wides.append(value * shift_cos - swap(value) * (sign * shift_sin))
    for k, model_ref in enumerate(model_refs):
        model_ref[...] = stage_ref[jnp.bitwise_xor(owner, k)]
    left = jnp.concatenate([wides[f][:, k * LANES : (k + 1) * LANES] for k in range(parts) for f in range(freqs)], axis=0)
    wide = matmul(jnp.concatenate(halves_of(left), axis=0), hot_ref[...], NN)
    wide = wide[:half] + wide[half:]
    for s in range(shots):
        for h in range(2):
            lanes = slice((2 * s + h) * LANES, (2 * s + h + 1) * LANES)
            key, _ = cells(s, h)
            for f in range(freqs):
                acc = jnp.zeros((8, LANES), F32)
                for k in range(parts):
                    first = (k * freqs + f) * 8
                    acc = acc + jnp.where(key == k, wide[first : first + 8, lanes], 0.0)
                acc = acc + pltpu.roll(acc, 1, 0)
                acc = acc + pltpu.roll(acc, 2, 0)
                out_ref[s * freqs + f, h : h + 1, :] = acc[3:4]
                out_ref[s * freqs + f, 2 + h : 3 + h, :] = acc[7:8]


HBM = pl.BlockSpec(memory_space=pltpu.HBM)
VMEM = pl.BlockSpec(memory_space=pltpu.VMEM)


def call(kernel, out_shape, scratch=(), specs=None):
    return pl.pallas_call(
        kernel,
        out_shape=out_shape,
        **({"in_specs": specs} if specs else {}),
        scratch_shapes=list(scratch),
        interpret=INTERPRET,
        compiler_params=pltpu.CompilerParams(vmem_limit_bytes=48 << 20),
    )


def shape_of(shape, dtype=F32):
    return jax.ShapeDtypeStruct(shape, dtype)


def per_device(traces, trace_slot, trace_cmp, trace_bin, prior_weight):
    trace_dev = traces.shape[2]
    shot_count = lax.axis_size("shot")
    freq_count = lax.axis_size("freq")
    freqs = traces.shape[0] * freq_count
    groups = shot_count * freq_count
    slot_total = 2 * trace_dev
    cap = slot_total // groups
    blocks = slot_total // BLOCK
    fields = traces[0]
    slot = trace_slot.reshape(1, -1)
    axes = ("shot", "freq")

    indices = pltpu.VMEM(slot.shape, jnp.int32)
    scratch = (pltpu.VMEM(fields.shape, F32), indices, indices, indices, pltpu.SemaphoreType.DMA((4,)))
    sent = call(route_kernel, shape_of((blocks, 8, LANES)), scratch, [HBM] * 4)(
        *held(fields, slot, trace_cmp.reshape(1, -1), trace_bin.reshape(1, -1))
    )
    fine = BLOCK // cap
    if fine > 1:
        sent = sent[:, :6].reshape(blocks, 3, fine, cap).transpose(0, 2, 1, 3).reshape(groups, 3, cap)
    arrived = lax.all_to_all(sent, axes, split_axis=0, concat_axis=0, tiled=True)
    if fine > 1:
        arrived = arrived.reshape(shot_count // fine, fine, freq_count, 3, cap).transpose(0, 2, 3, 1, 4)
        arrived = arrived.reshape(blocks, 6, LANES)
        arrived = jnp.pad(arrived, ((0, 0), (0, 2), (0, 0)))

    dft, twiddle = dft_constants()
    base = phase_constants(freqs)
    slots_dev = blocks // freqs * BLOCK
    rows = 3 * freqs * 8 * (BINS // LANES) + 8 * (BINS // LANES)
    field = shape_of((8, Q))
    returned, *models = call(
        solve_kernel,
        (shape_of((blocks, 4, LANES)), *[field] * freqs),
        (
            pltpu.VMEM((rows, slots_dev), BF16),
            pltpu.VMEM((LANES, slots_dev), BF16),
            pltpu.VMEM((freqs, 2 * Q, BINS), BF16),
            pltpu.VMEM((freqs, 2 * Q, BINS), BF16),
            pltpu.VMEM(base.shape, F32),
            pltpu.VMEM(dft.shape, BF16),
            pltpu.VMEM((freqs, 8, Q), F32),
            pltpu.SemaphoreType.DMA((2,)),
        ),
        [VMEM] * 3 + [HBM] * 2,
    )(arrived, prior_weight, twiddle, *held(base, dft))

    for k in range(1, freqs):
        models[k] = lax.ppermute(models[k], "freq", [(i, i ^ k) for i in range(freqs)])
    if fine > 1:
        returned = returned.reshape(shot_count // fine, freq_count, 2, fine, cap).transpose(0, 3, 1, 2, 4)
        returned = returned.reshape(groups, 2, cap)
    back = lax.all_to_all(returned, axes, split_axis=0, concat_axis=0, tiled=True)
    if fine > 1:
        back = back.reshape(blocks, fine, 2, cap).transpose(0, 2, 1, 3)
    primaries, radon = call(
        unroute_kernel,
        (shape_of(fields.shape), shape_of((2,) + prior_weight.shape)),
        (pltpu.VMEM((freqs, 8, Q), F32),),
    )(fields, slot, back.reshape(4 * blocks, LANES), *models)
    return primaries[None], radon[None]


def solution(mesh):
    return jax.shard_map(
        per_device,
        mesh=mesh,
        in_specs=(P("freq", None, "shot"), P("shot"), P("shot"), P("shot"), P("shot", None)),
        out_specs=(P("freq", None, "shot"), P("freq", None, "shot", None)),
        check_vma=False,
    )
```
